64 devices in a mesh: dp: 8 (over x, y, core), tp: 8 (over z).
Axes of the slice: x: 2, y: 2, z: 8, core: 2. Of those that a mesh axis runs over, the one named last changes fastest.
The devices are a block of a 4x4x8 slice.
Arguments:
- x: bfloat16 [16384, 2048], P('dp'), parts along dimension 0
- dy: bfloat16 [16384, 2048], P('dp'), parts along dimension 0
- gate: bfloat16 [16384, 8192], P('dp', 'tp'), parts along dimension 0
- up: bfloat16 [16384, 8192], P('dp', 'tp'), parts along dimension 0
- w_gate: bfloat16 [2048, 8192], P(None, 'tp')
- w_up: bfloat16 [2048, 8192], P(None, 'tp')
- w_down: bfloat16 [8192, 2048], P('tp')
Outputs:
- output 1: bfloat16 [16384, 2048], P('dp'), parts along dimension 0
- output 2: bfloat16 [16384, 8192], P('dp', 'tp'), parts along dimension 0
- output 3: bfloat16 [16384, 8192], P('dp', 'tp'), parts along dimension 0
- output 4: bfloat16 [65536, 2048], P(('dp', 'tp')), parts along dimension 0
There are 8 independent parts. The reference program is written for one: setup_inputs(seed, part) draws one part's arguments, and reference() takes and returns one part's arrays. A program takes and returns all parts, laid end to end along the dimension named above; an argument that names none is the same for every part.
All inputs are finite; a program needn't handle non-finite values.
Results may differ from the reference program's by a relative error of at most 0.012.
Values are sent between devices in bfloat16 or wider.
A program may use at most 768 MiB of HBM per device.

```python
import jax
import jax.numpy as jnp

ROWS = 2048
D = 2048
FF = 8192


def act(gate, up):
    return jax.nn.silu(gate) * up


def setup_inputs(seed: int = 0, part: int = 0) -> dict:
    kx, ky, ka, kb, kg, ku, kd = jax.random.split(jax.random.key(seed), 7)
    kx, ky, ka, kb = (jax.random.fold_in(k, part) for k in (kx, ky, ka, kb))
    drawn = {
        "x": jax.random.normal(kx, (ROWS, D), jnp.float32),
        "dy": jax.random.normal(ky, (ROWS, D), jnp.float32),
        "gate": jax.random.normal(ka, (ROWS, FF), jnp.float32),
        "up": jax.random.normal(kb, (ROWS, FF), jnp.float32),
        "w_gate": jax.random.normal(kg, (D, FF), jnp.float32) * D**-0.5,
        "w_up": jax.random.normal(ku, (D, FF), jnp.float32) * D**-0.5,
        "w_down": jax.random.normal(kd, (FF, D), jnp.float32) * FF**-0.5,
    }
    return {k: v.astype(jnp.bfloat16) for k, v in drawn.items()}


def reference(x, dy, gate, up, w_gate, w_up, w_down):
    hidden, back = jax.vjp(act, gate.astype(jnp.float32), up.astype(jnp.float32))
    d_hidden = jnp.dot(dy, w_down.T, preferred_element_type=jnp.float32)
    d_gate, d_up = (g.astype(jnp.bfloat16) for g in back(d_hidden))
    dx = jnp.dot(d_gate, w_gate.T, preferred_element_type=jnp.float32) + jnp.dot(d_up, w_up.T, preferred_element_type=jnp.float32)
    dw_gate = jnp.dot(x.T, d_gate, preferred_element_type=jnp.float32)
    dw_up = jnp.dot(x.T, d_up, preferred_element_type=jnp.float32)
    dw_down = jnp.dot(hidden.astype(jnp.bfloat16).T, dy, preferred_element_type=jnp.float32)
    return tuple(g.astype(jnp.bfloat16) for g in (dx, dw_gate, dw_up, dw_down))
```

```python
import functools

import jax
import jax.numpy as jnp
from jax import lax
from jax.experimental import pallas as pl
from jax.experimental.pallas import tpu as pltpu
from jax.sharding import PartitionSpec as P

RINGS = 8
CHUNKS = 4
TILE = 128
BF16, F32 = jnp.bfloat16, jnp.float32
NT = (((1,), (1,)), ((), ()))
TN = (((0,), (0,)), ((), ()))


def kernel(
    n,
    x,
    dy,
    gate,
    up,
    w_gate,
    w_up,
    w_down,
    dx,
    dw_gate,
    dw_up,
    dw_down,
    x_v,
    dy_v,
    dg_v,
    du_v,
    hid_v,
    wg_v,
    wu_v,
    wd_v,
    dx_v,
    slots,
    stage,
    in_sem,
    wd_sem,
    w_sem,
    x_sem,
    stage_sem,
    dx_sem,
    send_sem,
    rs_sem,
    ag_sem,
):
    tokens, depth = dy.shape
    hidden = gate.shape[1]
    rows, cols, fcols = tokens // n, depth // RINGS, hidden // CHUNKS
    me = lax.axis_index("tp")
    right, left = lax.rem(me + 1, n), lax.rem(me + n - 1, n)

    barrier = pltpu.get_barrier_semaphore()
    for neighbour in (left, right):
        pl.semaphore_signal(barrier, inc=1, device_id={"tp": neighbour}, device_id_type=pl.DeviceIdType.MESH)

    def block(b):
        return pl.ds(pl.multiple_of(b * rows, rows), rows)

    def strip(s):
        return pl.ds(pl.multiple_of(s * cols, cols), cols)

    def chunk(c):
        return pl.ds(pl.multiple_of(c * fcols, fcols), fcols)

    def tile(i):
        return pl.ds(pl.multiple_of(i * TILE, TILE), TILE)

    def rows_in(b):
        return [
            pltpu.make_async_copy(src.at[block(b), :], dst.at[block(b), :], in_sem.at[k, b])
            for k, (src, dst) in enumerate(((dy, dy_v), (gate, dg_v), (up, du_v)))
        ]

    def down_in(c):
        return pltpu.make_async_copy(w_down.at[chunk(c), :], wd_v.at[chunk(c), :], wd_sem.at[c])

    def strips_in(s):
        return [
            pltpu.make_async_copy(src.at[strip(s), :], dst.at[strip(s), :], w_sem.at[k, s])
            for k, (src, dst) in enumerate(((w_gate, wg_v), (w_up, wu_v)))
        ]

    x_in = pltpu.make_async_copy(x, x_v, x_sem)

    def right_block(t):
        return lax.rem(me + 2 * n - 1 - t, n)

    def left_block(t):
        return lax.rem(me + n - 1 + t, n)

    for copy in rows_in(right_block(0)):
        copy.start()
    for c in range(CHUNKS):
        down_in(c).start()

    @pl.loop(0, RINGS)
    def _(s):
        for copy in strips_in(s):
            copy.start()

    @pl.loop(1, n // 2)
    def _(t):
        for copy in rows_in(right_block(t)) + rows_in(left_block(t)):
            copy.start()

    for copy in rows_in(left_block(n // 2)):
        copy.start()
    x_in.start()

    def grads(b, c):
        at = (block(b), chunk(c))
        d_hidden = lax.dot_general(dy_v[block(b), :], wd_v[chunk(c), :], NT, preferred_element_type=F32)
        g, u = dg_v[at].astype(F32), du_v[at].astype(F32)
        sig = jax.nn.sigmoid(g)
        act = g * sig
        hid_v[at] = (act * u).astype(BF16)
        dg_v[at] = (d_hidden * u * (sig + act * (1.0 - sig))).astype(BF16)
        du_v[at] = (d_hidden * act).astype(BF16)

    def term(b, s):
        return lax.dot_general(dg_v[block(b), :], wg_v[strip(s), :], NT, preferred_element_type=F32) + lax.dot_general(
            du_v[block(b), :], wu_v[strip(s), :], NT, preferred_element_type=F32
        )

    def target(odd):
        return {"tp": left if odd else right}

    def rs_copy(s, odd, t):
        return pltpu.make_async_remote_copy(
            src_ref=slots.at[s, t],
            dst_ref=slots.at[s, t + 1],
            send_sem=send_sem.at[s],
            recv_sem=rs_sem.at[s, t],
            device_id=target(odd),
            device_id_type=pl.DeviceIdType.MESH,
        )

    def ag_block(odd, t):
        return lax.rem(me + n - 2 + t, n) if odd else lax.rem(me + n - t, n)

    def ag_copy(s, odd, t):
        here = dx_v.at[block(ag_block(odd, t)), strip(s)]
        return pltpu.make_async_remote_copy(
            src_ref=here,
            dst_ref=here,
            send_sem=send_sem.at[s],
            recv_sem=ag_sem.at[s, t],
            device_id=target(odd),
            device_id_type=pl.DeviceIdType.MESH,
        )

    def dx_out(s, odd, t):
        at = (block(ag_block(odd, t)), strip(s))
        return pltpu.make_async_copy(dx_v.at[at], dx.at[at], dx_sem)

    def send_first(s, odd):
        slots[s, 0] = term(right_block(0), s).astype(BF16)
        rs_copy(s, odd, 0).start()

    def pass_on(s, odd, t):
        rs_copy(s, odd, t - 1).wait_recv()
        b = left_block(t) if odd else right_block(t)
        slots[s, t] = (slots[s, t].astype(F32) + term(b, s)).astype(BF16)
        rs_copy(s, odd, t - 1).wait_send()
        rs_copy(s, odd, t).start()

    def finish(s, odd):
        t = n - 1
        rs_copy(s, odd, t - 1).wait_recv()
        b = left_block(t) if odd else right_block(t)
        dx_v[block(b), strip(s)] = (slots[s, t].astype(F32) + term(b, s)).astype(BF16)
        rs_copy(s, odd, t - 1).wait_send()
        ag_copy(s, odd, 0).start()
        dx_out(s, odd, 0).start()

    def hand_on(s, odd, t, last=False):
        before = t - 1
        arrived = pltpu.make_async_remote_copy(
            src_ref=dx_v.at[block(ag_block(odd, t)), strip(s)],
            dst_ref=dx_v.at[block(ag_block(odd, t)), strip(s)],
            send_sem=send_sem.at[s],
            recv_sem=ag_sem.at[s, before],
            device_id=target(odd),
            device_id_type=pl.DeviceIdType.MESH,
        )
        arrived.wait_recv()
        arrived.wait_send()
        if not last:
            ag_copy(s, odd, t).start()
        dx_out(s, odd, t).start()

    def stage_copies(i, slot, targets):
        width = stage.shape[-1] // len(targets)
        return [
            pltpu.make_async_copy(
                stage.at[slot, :, pl.ds(k * width, width)], dst.at[tile(i), :], stage_sem.at[k, slot]
            )
            for k, dst in enumerate(targets)
        ]

    def down_grad(i):
        slot = lax.rem(i, 2)

        @pl.when(i >= 2)
        def _():
            for copy in stage_copies(i - 2, slot, [dw_down]):
                copy.wait()

        stage[slot] = lax.dot_general(hid_v[:, tile(i)], dy_v[...], TN, preferred_element_type=F32).astype(BF16)
        for copy in stage_copies(i, slot, [dw_down]):
            copy.start()

    def up_grads(i):
        slot = lax.rem(i, 2)

        @pl.when(i >= 2)
        def _():
            for copy in stage_copies(i - 2, slot, [dw_gate, dw_up]):
                copy.wait()

        xt = x_v[:, tile(i)]
        stage[slot, :, :hidden] = lax.dot_general(xt, dg_v[...], TN, preferred_element_type=F32).astype(BF16)
        stage[slot, :, hidden:] = lax.dot_general(xt, du_v[...], TN, preferred_element_type=F32).astype(BF16)
        for copy in stage_copies(i, slot, [dw_gate, dw_up]):
            copy.start()

    for copy in rows_in(right_block(0)):
        copy.wait()

    @pl.loop(0, CHUNKS)
    def _(c):
        down_in(c).wait()
        grads(right_block(0), c)

    pl.semaphore_wait(barrier, 2)
    pairs = RINGS // 2
    per_pair = 2 * CHUNKS // pairs

    @pl.loop(0, pairs)
    def _(j):
        for odd in range(2):
            for copy in strips_in(2 * j + odd):
                copy.wait()
            send_first(2 * j + odd, odd)

    def arrive(b):
        for copy in rows_in(b):
            copy.wait()

    arrive(right_block(1))

    @pl.loop(0, CHUNKS)
    def _(c):
        grads(right_block(1), c)

    arrive(left_block(1))

    @pl.loop(0, CHUNKS)
    def _(c):
        grads(left_block(1), c)

    half = n // 2

    @pl.loop(1, half - 1)
    def _(t):
        arrive(right_block(t + 1))
        arrive(left_block(t + 1))

        @pl.loop(0, pairs)
        def _(j):
            pass_on(2 * j, 0, t)
            grads(right_block(t + 1), j)
            pass_on(2 * j + 1, 1, t)
            grads(left_block(t + 1), j)

    arrive(left_block(half))

    @pl.loop(0, pairs)
    def _(j):
        pass_on(2 * j, 0, half - 1)
        grads(left_block(half), j)
        pass_on(2 * j + 1, 1, half - 1)

    @pl.loop(half, n - 1)
    def _(t):
        @pl.loop(0, pairs)
        def _(j):
            pass_on(2 * j, 0, t)
            pass_on(2 * j + 1, 1, t)
            i = (t - half) * pairs + j

            @pl.when(i < hidden // TILE)
            def _():
                down_grad(i)

    for i in range(hidden // TILE - 2, hidden // TILE):
        for copy in stage_copies(i, i % 2, [dw_down]):
            copy.wait()
    x_in.wait()

    @pl.loop(0, pairs)
    def _(j):
        finish(2 * j, 0)
        finish(2 * j + 1, 1)

    @pl.loop(1, n - 1)
    def _(t):
        @pl.loop(0, pairs)
        def _(j):
            hand_on(2 * j, 0, t)
            hand_on(2 * j + 1, 1, t)
            i = (t - 1) * pairs + j

            @pl.when(i < depth // TILE)
            def _():
                up_grads(i)

    for i in range(depth // TILE - 2, depth // TILE):
        for copy in stage_copies(i, i % 2, [dw_gate, dw_up]):
            copy.wait()

    @pl.loop(0, pairs)
    def _(j):
        hand_on(2 * j, 0, n - 1, last=True)
        hand_on(2 * j + 1, 1, n - 1, last=True)

    pltpu.make_async_copy(dx_v, dx, dx_sem).wait()


def solution(mesh):
    n = mesh.shape["tp"]

    def step(x, dy, gate, up, w_gate, w_up, w_down):
        tokens, depth = dy.shape
        hidden = gate.shape[1]
        rows, cols = tokens // n, depth // RINGS
        hbm = pl.BlockSpec(memory_space=pltpu.HBM)
        dma = pltpu.SemaphoreType.DMA
        return pl.pallas_call(
            functools.partial(kernel, n),
            name="mlp_backward",
            out_shape=[
                jax.ShapeDtypeStruct((tokens, depth), BF16),
                jax.ShapeDtypeStruct((depth, hidden), BF16),
                jax.ShapeDtypeStruct((depth, hidden), BF16),
                jax.ShapeDtypeStruct((hidden, depth), BF16),
            ],
            in_specs=[hbm] * 7,
            out_specs=[hbm] * 4,
            scratch_shapes=[
                pltpu.VMEM((tokens, depth), BF16),
                pltpu.VMEM((tokens, depth), BF16),
                pltpu.VMEM((tokens, hidden), BF16),
                pltpu.VMEM((tokens, hidden), BF16),
                pltpu.VMEM((tokens, hidden), BF16),
                pltpu.VMEM((depth, hidden), BF16),
                pltpu.VMEM((depth, hidden), BF16),
                pltpu.VMEM((hidden, depth), BF16),
                pltpu.VMEM((tokens, depth), BF16),
                pltpu.VMEM((RINGS, n, rows, cols), BF16),
                pltpu.VMEM((2, TILE, 2 * hidden), BF16),
                dma((3, n)),
                dma((CHUNKS,)),
                dma((2, RINGS)),
                dma,
                dma((2, 2)),
                dma,
                dma((RINGS,)),
                dma((RINGS, n)),
                dma((RINGS, n)),
            ],
            compiler_params=pltpu.CompilerParams(
                collective_id=0,
                has_side_effects=True,
                vmem_limit_bytes=67_043_328,
                fuse_transposed_lhs_in_matmul=True,
            ),
            cost_estimate=pl.CostEstimate(
                flops=12 * tokens * depth * hidden, bytes_accessed=14 * tokens * depth * 2, transcendentals=0
            ),
        )(x, dy, gate, up, w_gate, w_up, w_down)

    tokens, columns, rows = P("dp", None), P(None, "tp"), P("tp", None)
    return jax.shard_map(
        step,
        mesh=mesh,
        in_specs=(tokens, tokens, P("dp", "tp"), P("dp", "tp"), columns, columns, rows),
        out_specs=(tokens, P("dp", "tp"), P("dp", "tp"), P(("dp", "tp"), None)),
        check_vma=False,
    )
```

```python
import functools

import jax
import jax.numpy as jnp
from jax import lax
from jax.experimental import pallas as pl
from jax.experimental.pallas import tpu as pltpu
from jax.sharding import PartitionSpec as P

RINGS = 8
CHUNKS = 4
TILE = 128
BF16, F32 = jnp.bfloat16, jnp.float32
NT = (((1,), (1,)), ((), ()))
TN = (((0,), (0,)), ((), ()))


def kernel(
    n,
    x,
    dy,
    gate,
    up,
    w_gate,
    w_up,
    w_down,
    dx,
    dw_gate,
    dw_up,
    dw_down,
    dy_v,
    dg_v,
    du_v,
    hid_v,
    wg_v,
    wu_v,
    wd_v,
    slots,
    in_sem,
    wd_sem,
    w_sem,
    x_sem,
    send_sem,
    rs_sem,
    ag_sem,
):
    tokens, depth = dy.shape
    hidden = gate.shape[1]
    rows, cols, fcols = tokens // n, depth // RINGS, hidden // CHUNKS
    me = lax.axis_index("tp")
    right, left = lax.rem(me + 1, n), lax.rem(me + n - 1, n)

    barrier = pltpu.get_barrier_semaphore()
    for neighbour in (left, right):
        pl.semaphore_signal(barrier, inc=1, device_id={"tp": neighbour}, device_id_type=pl.DeviceIdType.MESH)

    def block(b):
        return pl.ds(pl.multiple_of(b * rows, rows), rows)

    def strip(s):
        return pl.ds(pl.multiple_of(s * cols, cols), cols)

    def chunk(c):
        return pl.ds(pl.multiple_of(c * fcols, fcols), fcols)

    def tile(i):
        return pl.ds(pl.multiple_of(i * TILE, TILE), TILE)

    def rows_in(b):
        return [
            pltpu.make_async_copy(src.at[block(b), :], dst.at[block(b), :], in_sem.at[k, b])
            for k, (src, dst) in enumerate(((dy, dy_v), (gate, dg_v), (up, du_v)))
        ]

    def down_in(c):
        return pltpu.make_async_copy(w_down.at[chunk(c), :], wd_v.at[chunk(c), :], wd_sem.at[c])

    def strips_in(s):
        return [
            pltpu.make_async_copy(src.at[strip(s), :], dst.at[strip(s), :], w_sem.at[k, s])
            for k, (src, dst) in enumerate(((w_gate, wg_v), (w_up, wu_v)))
        ]

    halves = [(wg_v, 0), (wu_v, hidden)]

    def x_in(k):
        dst, first = halves[k]
        return pltpu.make_async_copy(x.at[:, pl.ds(first, hidden)], dst, x_sem.at[k])


    def right_block(t):
        return lax.rem(me + 2 * n - 1 - t, n)

    def left_block(t):
        return lax.rem(me + n - 1 + t, n)

    for copy in rows_in(right_block(0)):
        copy.start()
    for c in range(CHUNKS):
        down_in(c).start()

    @pl.loop(0, RINGS)
    def _(s):
        for copy in strips_in(s):
            copy.start()

    @pl.loop(1, n // 2)
    def _(t):
        for copy in rows_in(right_block(t)) + rows_in(left_block(t)):
            copy.start()

    for copy in rows_in(left_block(n // 2)):
        copy.start()

    def grads(b, c):
        at = (block(b), chunk(c))
        d_hidden = lax.dot_general(dy_v[block(b), :], wd_v[chunk(c), :], NT, preferred_element_type=F32)
        g, u = dg_v[at].astype(F32), du_v[at].astype(F32)
        sig = jax.nn.sigmoid(g)
        act = g * sig
        hid_v[at] = (act * u).astype(BF16)
        dg_v[at] = (d_hidden * u * (sig + act * (1.0 - sig))).astype(BF16)
        du_v[at] = (d_hidden * act).astype(BF16)

    def term(b, s):
        return lax.dot_general(dg_v[block(b), :], wg_v[strip(s), :], NT, preferred_element_type=F32) + lax.dot_general(
            du_v[block(b), :], wu_v[strip(s), :], NT, preferred_element_type=F32
        )

    def target(odd):
        return {"tp": left if odd else right}

    def rs_copy(s, odd, t):
        return pltpu.make_async_remote_copy(
            src_ref=slots.at[s, t],
            dst_ref=slots.at[s, t + 1],
            send_sem=send_sem.at[s],
            recv_sem=rs_sem.at[s, t],
            device_id=target(odd),
            device_id_type=pl.DeviceIdType.MESH,
        )

    def ag_block(odd, t):
        return lax.rem(me + n - 2 + t, n) if odd else lax.rem(me + n - t, n)

    def ag_copy(s, odd, t):
        here = dx.at[block(ag_block(odd, t)), strip(s)]
        return pltpu.make_async_remote_copy(
            src_ref=here,
            dst_ref=here,
            send_sem=send_sem.at[s],
            recv_sem=ag_sem.at[s, t],
            device_id=target(odd),
            device_id_type=pl.DeviceIdType.MESH,
        )

    def send_first(s, odd):
        slots[s, 0] = term(right_block(0), s).astype(BF16)
        rs_copy(s, odd, 0).start()

    def pass_on(s, odd, t):
        rs_copy(s, odd, t - 1).wait_recv()
        b = left_block(t) if odd else right_block(t)
        slots[s, t] = (slots[s, t].astype(F32) + term(b, s)).astype(BF16)
        rs_copy(s, odd, t - 1).wait_send()
        rs_copy(s, odd, t).start()

    def finish(s, odd):
        t = n - 1
        rs_copy(s, odd, t - 1).wait_recv()
        b = left_block(t) if odd else right_block(t)
        dx[block(b), strip(s)] = (slots[s, t].astype(F32) + term(b, s)).astype(BF16)
        rs_copy(s, odd, t - 1).wait_send()
        ag_copy(s, odd, 0).start()

    def hand_on(s, odd, t, last=False):
        before = t - 1
        arrived = pltpu.make_async_remote_copy(
            src_ref=dx.at[block(ag_block(odd, t)), strip(s)],
            dst_ref=dx.at[block(ag_block(odd, t)), strip(s)],
            send_sem=send_sem.at[s],
            recv_sem=ag_sem.at[s, before],
            device_id=target(odd),
            device_id_type=pl.DeviceIdType.MESH,
        )
        arrived.wait_recv()
        arrived.wait_send()
        if not last:
            ag_copy(s, odd, t).start()

    def down_grad(i):
        dw_down[tile(i), :] = lax.dot_general(hid_v[:, tile(i)], dy_v[...], TN, preferred_element_type=F32).astype(BF16)

    def up_grads(k, i):
        held, first = halves[k]
        xt = held[:, tile(i)]
        at = pl.ds(pl.multiple_of(first + i * TILE, TILE), TILE)
        dw_gate[at, :] = lax.dot_general(xt, dg_v[...], TN, preferred_element_type=F32).astype(BF16)
        dw_up[at, :] = lax.dot_general(xt, du_v[...], TN, preferred_element_type=F32).astype(BF16)

    for copy in rows_in(right_block(0)):
        copy.wait()

    @pl.loop(0, CHUNKS)
    def _(c):
        down_in(c).wait()
        grads(right_block(0), c)

    pl.semaphore_wait(barrier, 2)
    pairs = RINGS // 2
    per_pair = 2 * CHUNKS // pairs

    @pl.loop(0, pairs)
    def _(j):
        for odd in range(2):
            for copy in strips_in(2 * j + odd):
                copy.wait()
            send_first(2 * j + odd, odd)

    def arrive(b):
        for copy in rows_in(b):
            copy.wait()

    arrive(right_block(1))

    @pl.loop(0, CHUNKS)
    def _(c):
        grads(right_block(1), c)

    arrive(left_block(1))

    @pl.loop(0, CHUNKS)
    def _(c):
        grads(left_block(1), c)

    half = n // 2

    @pl.loop(1, half - 1)
    def _(t):
        arrive(right_block(t + 1))
        arrive(left_block(t + 1))

        @pl.loop(0, pairs)
        def _(j):
            pass_on(2 * j, 0, t)
            grads(right_block(t + 1), j)
            pass_on(2 * j + 1, 1, t)
            grads(left_block(t + 1), j)

    arrive(left_block(half))

    @pl.loop(0, pairs)
    def _(j):
        pass_on(2 * j, 0, half - 1)
        grads(left_block(half), j)
        pass_on(2 * j + 1, 1, half - 1)

    @pl.loop(half, n - 1)
    def _(t):
        @pl.loop(0, pairs)
        def _(j):
            pass_on(2 * j, 0, t)
            pass_on(2 * j + 1, 1, t)
            i = (t - half) * pairs + j

            @pl.when(i < hidden // TILE)
            def _():
                down_grad(i)

    @pl.loop(0, pairs)
    def _(j):
        finish(2 * j, 0)
        finish(2 * j + 1, 1)

    for k in range(2):
        x_in(k).start()

    def hand_on_all(t, last=False, also=None):
        @pl.loop(0, pairs)
        def _(j):
            hand_on(2 * j, 0, t, last)
            hand_on(2 * j + 1, 1, t, last)
            if also is not None:
                also(j)

    hand_on_all(1)
    steps = hidden // TILE // pairs
    for k in range(2):
        x_in(k).wait()

        @pl.loop(0, steps)
        def _(t):
            hand_on_all(2 + k * steps + t, also=lambda j: up_grads(k, t * pairs + j))

    @pl.loop(2 + 2 * steps, n - 1)
    def _(t):
        hand_on_all(t)

    hand_on_all(n - 1, last=True)


def write_out(*refs):
    sources, targets, sem = refs[:4], refs[4:8], refs[8]
    copies = [pltpu.make_async_copy(src, dst, sem.at[k]) for k, (src, dst) in enumerate(zip(sources, targets))]
    for copy in copies:
        copy.start()
    for copy in copies:
        copy.wait()


def solution(mesh):
    n = mesh.shape["tp"]

    def step(x, dy, gate, up, w_gate, w_up, w_down):
        tokens, depth = dy.shape
        hidden = gate.shape[1]
        rows, cols = tokens // n, depth // RINGS
        hbm = pl.BlockSpec(memory_space=pltpu.HBM)
        dma = pltpu.SemaphoreType.DMA
        shapes = [(tokens, depth), (depth, hidden), (depth, hidden), (hidden, depth)]
        vmem = pl.BlockSpec(memory_space=pltpu.VMEM)
        held = pl.pallas_call(
            functools.partial(kernel, n),
            name="mlp_backward",
            out_shape=[pltpu.VMEM(shape, BF16) for shape in shapes],
            in_specs=[hbm] * 7,
            out_specs=[vmem] * 4,
            scratch_shapes=[
                pltpu.VMEM((tokens, depth), BF16),
                pltpu.VMEM((tokens, hidden), BF16),
                pltpu.VMEM((tokens, hidden), BF16),
                pltpu.VMEM((tokens, hidden), BF16),
                pltpu.VMEM((depth, hidden), BF16),
                pltpu.VMEM((depth, hidden), BF16),
                pltpu.VMEM((hidden, depth), BF16),
                pltpu.VMEM((RINGS, n, rows, cols), BF16),
                dma((3, n)),
                dma((CHUNKS,)),
                dma((2, RINGS)),
                dma((2,)),
                dma((RINGS,)),
                dma((RINGS, n)),
                dma((RINGS, n)),
            ],
            compiler_params=pltpu.CompilerParams(
                collective_id=0, has_side_effects=True, vmem_limit_bytes=45_000_000
            ),
            cost_estimate=pl.CostEstimate(
                flops=12 * tokens * depth * hidden, bytes_accessed=14 * tokens * depth * 2, transcendentals=0
            ),
        )(x, dy, gate, up, w_gate, w_up, w_down)
        return pl.pallas_call(
            write_out,
            name="write_out",
            out_shape=[jax.ShapeDtypeStruct(shape, BF16) for shape in shapes],
            in_specs=[vmem] * 4,
            out_specs=[hbm] * 4,
            scratch_shapes=[dma((4,))],
            compiler_params=pltpu.CompilerParams(vmem_limit_bytes=1_000_000),
        )(*held)

    tokens, columns, rows = P("dp", None), P(None, "tp"), P("tp", None)
    return jax.shard_map(
        step,
        mesh=mesh,
        in_specs=(tokens, tokens, P("dp", "tp"), P("dp", "tp"), columns, columns, rows),
        out_specs=(tokens, P("dp", "tp"), P("dp", "tp"), P(("dp", "tp"), None)),
        check_vma=False,
    )
```

```python
import functools

import jax
import jax.numpy as jnp
from jax import lax
from jax.experimental import pallas as pl
from jax.experimental.pallas import tpu as pltpu
from jax.sharding import PartitionSpec as P

RINGS = 8
CHUNKS = 4
TILE = 128
BF16, F32 = jnp.bfloat16, jnp.float32
NT = (((1,), (1,)), ((), ()))
TN = (((0,), (0,)), ((), ()))


def kernel(
    n,
    x,
    dy,
    gate,
    up,
    w_gate,
    w_up,
    w_down,
    dx,
    tail_right,
    tail_left,
    dw_gate,
    dw_up,
    dw_down,
    dy_v,
    dg_v,
    du_v,
    hid_v,
    wg_v,
    wu_v,
    wd_v,
    slots,
    in_sem,
    wd_sem,
    w_sem,
    x_sem,
    send_sem,
    rs_sem,
    ag_sem,
):
    tokens, depth = dy.shape
    hidden = gate.shape[1]
    rows, cols, fcols = tokens // n, depth // RINGS, hidden // CHUNKS
    me = lax.axis_index("tp")
    right, left = lax.rem(me + 1, n), lax.rem(me + n - 1, n)

    barrier = pltpu.get_barrier_semaphore()
    for neighbour in (left, right):
        pl.semaphore_signal(barrier, inc=1, device_id={"tp": neighbour}, device_id_type=pl.DeviceIdType.MESH)

    def block(b):
        return pl.ds(pl.multiple_of(b * rows, rows), rows)

    def strip(s):
        return pl.ds(pl.multiple_of(s * cols, cols), cols)

    def chunk(c):
        return pl.ds(pl.multiple_of(c * fcols, fcols), fcols)

    def tile(i):
        return pl.ds(pl.multiple_of(i * TILE, TILE), TILE)

    def rows_in(b):
        return [
            pltpu.make_async_copy(src.at[block(b), :], dst.at[block(b), :], in_sem.at[k, b])
            for k, (src, dst) in enumerate(((dy, dy_v), (gate, dg_v), (up, du_v)))
        ]

    def down_in(c):
        return pltpu.make_async_copy(w_down.at[chunk(c), :], wd_v.at[chunk(c), :], wd_sem.at[c])

    def strips_in(s):
        return [
            pltpu.make_async_copy(src.at[strip(s), :], dst.at[strip(s), :], w_sem.at[k, s])
            for k, (src, dst) in enumerate(((w_gate, wg_v), (w_up, wu_v)))
        ]

    halves = [(wg_v, 0), (wu_v, hidden)]

    def x_in(k):
        dst, first = halves[k]
        return pltpu.make_async_copy(x.at[:, pl.ds(first, hidden)], dst, x_sem.at[k])


    def right_block(t):
        return lax.rem(me + 2 * n - 1 - t, n)

    def left_block(t):
        return lax.rem(me + n - 1 + t, n)

    for copy in rows_in(right_block(0)):
        copy.start()
    for c in range(CHUNKS):
        down_in(c).start()

    pairs = RINGS // 2

    @pl.loop(0, pairs)
    def _(j):
        for copy in strips_in(j) + strips_in(pairs + j):
            copy.start()

    @pl.loop(1, n // 2)
    def _(t):
        for copy in rows_in(right_block(t)) + rows_in(left_block(t)):
            copy.start()

    for copy in rows_in(left_block(n // 2)):
        copy.start()

    def grads(b, c):
        at = (block(b), chunk(c))
        d_hidden = lax.dot_general(dy_v[block(b), :], wd_v[chunk(c), :], NT, preferred_element_type=F32)
        g, u = dg_v[at].astype(F32), du_v[at].astype(F32)
        sig = jax.nn.sigmoid(g)
        act = g * sig
        hid_v[at] = (act * u).astype(BF16)
        dg_v[at] = (d_hidden * u * (sig + act * (1.0 - sig))).astype(BF16)
        du_v[at] = (d_hidden * act).astype(BF16)

    def term(b, s):
        return lax.dot_general(dg_v[block(b), :], wg_v[strip(s), :], NT, preferred_element_type=F32) + lax.dot_general(
            du_v[block(b), :], wu_v[strip(s), :], NT, preferred_element_type=F32
        )

    def target(odd):
        return {"tp": left if odd else right}

    def rs_copy(s, odd, t):
        return pltpu.make_async_remote_copy(
            src_ref=slots.at[s, t],
            dst_ref=slots.at[s, t + 1],
            send_sem=send_sem.at[s],
            recv_sem=rs_sem.at[s, t],
            device_id=target(odd),
            device_id_type=pl.DeviceIdType.MESH,
        )

    def ag_block(odd, t):
        return gather_block(n, me, odd, t)

    def ag_copy(s, odd, t):
        here = dx.at[block(ag_block(odd, t)), strip(s)]
        return ag_to(s, odd, t, here, here)

    def ag_to(s, odd, t, src, dst):
        return pltpu.make_async_remote_copy(
            src_ref=src,
            dst_ref=dst,
            send_sem=send_sem.at[s],
            recv_sem=ag_sem.at[s, t],
            device_id=target(odd),
            device_id_type=pl.DeviceIdType.MESH,
        )

    def ag_last_copy(s, odd):
        t = n - 3
        dst = (tail_left if odd else tail_right).at[:, strip(s - odd * pairs)]
        return ag_to(s, odd, t, dx.at[block(ag_block(odd, t)), strip(s)], dst)

    def send_first(s, odd):
        slots[s, 0] = term(right_block(0), s).astype(BF16)
        rs_copy(s, odd, 0).start()

    def pass_on(s, odd, t):
        rs_copy(s, odd, t - 1).wait_recv()
        b = left_block(t) if odd else right_block(t)
        slots[s, t] = (slots[s, t].astype(F32) + term(b, s)).astype(BF16)
        rs_copy(s, odd, t - 1).wait_send()
        rs_copy(s, odd, t).start()

    def finish(s, odd):
        t = n - 1
        rs_copy(s, odd, t - 1).wait_recv()
        b = left_block(t) if odd else right_block(t)
        dx[block(b), strip(s)] = (slots[s, t].astype(F32) + term(b, s)).astype(BF16)
        rs_copy(s, odd, t - 1).wait_send()
        ag_copy(s, odd, 0).start()

    def hand_on(s, odd, t):
        here = dx.at[block(ag_block(odd, t)), strip(s)]
        arrived = ag_to(s, odd, t - 1, here, here)
        arrived.wait_recv()
        arrived.wait_send()

        @pl.when(t < n - 3)
        def _():
            ag_copy(s, odd, t).start()

        @pl.when(t == n - 3)
        def _():
            ag_last_copy(s, odd).start()

    def down_grad(i):
        dw_down[tile(i), :] = lax.dot_general(hid_v[:, tile(i)], dy_v[...], TN, preferred_element_type=F32).astype(BF16)

    def up_grads(k, i):
        held, first = halves[k]
        xt = held[:, tile(i)]
        at = pl.ds(pl.multiple_of(first + i * TILE, TILE), TILE)
        dw_gate[at, :] = lax.dot_general(xt, dg_v[...], TN, preferred_element_type=F32).astype(BF16)
        dw_up[at, :] = lax.dot_general(xt, du_v[...], TN, preferred_element_type=F32).astype(BF16)

    for copy in rows_in(right_block(0)):
        copy.wait()

    @pl.loop(0, CHUNKS)
    def _(c):
        down_in(c).wait()
        grads(right_block(0), c)

    pl.semaphore_wait(barrier, 2)

    @pl.loop(0, pairs)
    def _(j):
        for odd in range(2):
            for copy in strips_in(odd * pairs + j):
                copy.wait()
            send_first(odd * pairs + j, odd)

    def arrive(b):
        for copy in rows_in(b):
            copy.wait()

    arrive(right_block(1))

    @pl.loop(0, CHUNKS)
    def _(c):
        grads(right_block(1), c)

    arrive(left_block(1))

    @pl.loop(0, CHUNKS)
    def _(c):
        grads(left_block(1), c)

    half = n // 2

    @pl.loop(1, half - 1)
    def _(t):
        arrive(right_block(t + 1))
        arrive(left_block(t + 1))

        @pl.loop(0, pairs)
        def _(j):
            pass_on(j, 0, t)
            grads(right_block(t + 1), j)
            pass_on(pairs + j, 1, t)
            grads(left_block(t + 1), j)

    arrive(left_block(half))

    @pl.loop(0, pairs)
    def _(j):
        pass_on(j, 0, half - 1)
        grads(left_block(half), j)
        pass_on(pairs + j, 1, half - 1)

    @pl.loop(half, n - 1)
    def _(t):
        @pl.loop(0, pairs)
        def _(j):
            pass_on(j, 0, t)
            pass_on(pairs + j, 1, t)
            i = (t - half) * pairs + j

            @pl.when(i < hidden // TILE)
            def _():
                down_grad(i)

    @pl.loop(0, pairs)
    def _(j):
        finish(j, 0)
        finish(pairs + j, 1)

    for k in range(2):
        x_in(k).start()

    def hand_on_all(t, also=None):
        @pl.loop(0, pairs)
        def _(j):
            hand_on(j, 0, t)
            hand_on(pairs + j, 1, t)
            if also is not None:
                also(j)

    hand_on_all(1)
    steps = hidden // TILE // pairs
    for k in range(2):
        x_in(k).wait()

        @pl.loop(0, steps)
        def _(t):
            hand_on_all(2 + k * steps + t, also=lambda j: up_grads(k, t * pairs + j))

    @pl.loop(0, pairs)
    def _(j):
        for odd in range(2):
            last = ag_last_copy(odd * pairs + j, odd)
            last.wait_recv()
            last.wait_send()


def gather_block(n, me, odd, t):
    return lax.rem(me + n - 2 + t, n) if odd else lax.rem(me + n - t, n)


def move(pairs_of_refs, sem):
    copies = [pltpu.make_async_copy(src, dst, sem.at[k]) for k, (src, dst) in enumerate(pairs_of_refs)]
    for copy in copies:
        copy.start()
    for copy in copies:
        copy.wait()


def place(n, ref, odd, t):
    rows, cols = ref.shape[0] // n, ref.shape[1] // 2
    b = gather_block(n, lax.axis_index("tp"), odd, t)
    return ref.at[pl.ds(pl.multiple_of(b * rows, rows), rows), pl.ds(odd * cols, cols)]


def write_out(n, dx_v, tail_right, tail_left, dw_gate_v, dw_up_v, dw_down_v, dx, dw_gate, dw_up, dw_down, sem):
    moves = [(dw_gate_v, dw_gate), (dw_up_v, dw_up), (dw_down_v, dw_down)]
    for odd, tail in enumerate((tail_right, tail_left)):
        moves += [(place(n, dx_v, odd, t), place(n, dx, odd, t)) for t in range(n - 2)]
        moves.append((tail, place(n, dx, odd, n - 2)))
    move(moves, sem)


def put_last(n, _, from_left, from_right, dx, sem):
    move([(from_left, place(n, dx, 0, n - 1)), (from_right, place(n, dx, 1, n - 1))], sem)


def solution(mesh):
    n = mesh.shape["tp"]

    def step(x, dy, gate, up, w_gate, w_up, w_down):
        tokens, depth = dy.shape
        hidden = gate.shape[1]
        rows, cols = tokens // n, depth // RINGS
        hbm = pl.BlockSpec(memory_space=pltpu.HBM)
        dma = pltpu.SemaphoreType.DMA
        shapes = [(tokens, depth), (depth, hidden), (depth, hidden), (hidden, depth)]
        tail = (rows, depth // 2)
        vmem = pl.BlockSpec(memory_space=pltpu.VMEM)
        held = pl.pallas_call(
            functools.partial(kernel, n),
            name="mlp_backward",
            out_shape=[pltpu.VMEM(shape, BF16) for shape in (shapes[0], tail, tail, *shapes[1:])],
            in_specs=[hbm] * 7,
            out_specs=[vmem] * 6,
            scratch_shapes=[
                pltpu.VMEM((tokens, depth), BF16),
                pltpu.VMEM((tokens, hidden), BF16),
                pltpu.VMEM((tokens, hidden), BF16),
                pltpu.VMEM((tokens, hidden), BF16),
                pltpu.VMEM((depth, hidden), BF16),
                pltpu.VMEM((depth, hidden), BF16),
                pltpu.VMEM((hidden, depth), BF16),
                pltpu.VMEM((RINGS, n, rows, cols), BF16),
                dma((3, n)),
                dma((CHUNKS,)),
                dma((2, RINGS)),
                dma((2,)),
                dma((RINGS,)),
                dma((RINGS, n)),
                dma((RINGS, n)),
            ],
            compiler_params=pltpu.CompilerParams(
                collective_id=0, has_side_effects=True, vmem_limit_bytes=44_500_000
            ),
            cost_estimate=pl.CostEstimate(
                flops=12 * tokens * depth * hidden, bytes_accessed=14 * tokens * depth * 2, transcendentals=0
            ),
        )(x, dy, gate, up, w_gate, w_up, w_down)
        around = range(n)
        from_left = lax.ppermute(held[1], "tp", [(i, (i + 1) % n) for i in around])
        from_right = lax.ppermute(held[2], "tp", [(i, (i - 1) % n) for i in around])
        dx, *grads = pl.pallas_call(
            functools.partial(write_out, n),
            name="write_out",
            out_shape=[jax.ShapeDtypeStruct(shape, BF16) for shape in shapes],
            in_specs=[vmem] * 6,
            out_specs=[hbm] * 4,
            scratch_shapes=[dma((2 * n + 1,))],
            compiler_params=pltpu.CompilerParams(vmem_limit_bytes=1_000_000),
            cost_estimate=pl.CostEstimate(
                flops=tokens * depth * hidden, bytes_accessed=5 * tokens * depth * 2, transcendentals=0
            ),
        )(*held)
        dx = pl.pallas_call(
            functools.partial(put_last, n),
            name="put_last",
            out_shape=jax.ShapeDtypeStruct(shapes[0], BF16),
            in_specs=[hbm, vmem, vmem],
            out_specs=hbm,
            input_output_aliases={0: 0},
            scratch_shapes=[dma((2,))],
            compiler_params=pltpu.CompilerParams(vmem_limit_bytes=1_000_000),
        )(dx, from_left, from_right)
        return dx, *grads

    tokens, columns, rows = P("dp", None), P(None, "tp"), P("tp", None)
    return jax.shard_map(
        step,
        mesh=mesh,
        in_specs=(tokens, tokens, P("dp", "tp"), P("dp", "tp"), columns, columns, rows),
        out_specs=(tokens, P("dp", "tp"), P("dp", "tp"), P(("dp", "tp"), None)),
        check_vma=False,
    )
```

```python
import functools

import jax
import jax.numpy as jnp
from jax import lax
from jax.experimental import pallas as pl
from jax.experimental.pallas import tpu as pltpu
from jax.sharding import PartitionSpec as P

RINGS = 8
CHUNKS = 4
TILE = 128
BF16, F32 = jnp.bfloat16, jnp.float32
NT = (((1,), (1,)), ((), ()))
TN = (((0,), (0,)), ((), ()))


def kernel(
    n,
    x,
    dy,
    gate,
    up,
    w_gate,
    w_up,
    w_down,
    dx,
    tail_right,
    tail_left,
    dw_gate,
    dw_up,
    dw_down,
    dy_v,
    dg_v,
    du_v,
    hid_v,
    wg_v,
    wu_v,
    wd_v,
    slots,
    in_sem,
    wd_sem,
    w_sem,
    x_sem,
    send_sem,
    rs_sem,
    ag_sem,
):
    tokens, depth = dy.shape
    hidden = gate.shape[1]
    rows, cols, fcols = tokens // n, depth // RINGS, hidden // CHUNKS
    me = lax.axis_index("tp")
    right, left = lax.rem(me + 1, n), lax.rem(me + n - 1, n)

    barrier = pltpu.get_barrier_semaphore()
    for neighbour in (left, right):
        pl.semaphore_signal(barrier, inc=1, device_id={"tp": neighbour}, device_id_type=pl.DeviceIdType.MESH)

    def block(b):
        return pl.ds(pl.multiple_of(b * rows, rows), rows)

    def strip(s):
        return pl.ds(pl.multiple_of(s * cols, cols), cols)

    def chunk(c):
        return pl.ds(pl.multiple_of(c * fcols, fcols), fcols)

    def tile(i):
        return pl.ds(pl.multiple_of(i * TILE, TILE), TILE)

    def rows_in(b):
        return [
            pltpu.make_async_copy(src.at[block(b), :], dst.at[block(b), :], in_sem.at[k, b])
            for k, (src, dst) in enumerate(((gate, dg_v), (up, du_v), (dy, dy_v)))
        ]

    def down_in(c):
        return pltpu.make_async_copy(w_down.at[chunk(c), :], wd_v.at[chunk(c), :], wd_sem.at[c])

    def strips_in(s):
        return [
            pltpu.make_async_copy(src.at[strip(s), :], dst.at[strip(s), :], w_sem.at[k, s])
            for k, (src, dst) in enumerate(((w_gate, wg_v), (w_up, wu_v)))
        ]

    halves = [(wg_v, 0), (wu_v, hidden)]

    def x_in(k):
        dst, first = halves[k]
        return pltpu.make_async_copy(x.at[:, pl.ds(first, hidden)], dst, x_sem.at[k])


    def right_block(t):
        return lax.rem(me + 2 * n - 1 - t, n)

    def left_block(t):
        return lax.rem(me + n - 1 + t, n)

    first = rows_in(right_block(0))
    for copy in first:
        copy.start()
    down_in(0).start()

    pairs = RINGS // 2

    def start_rest():
        @pl.loop(0, pairs)
        def _(j):
            for copy in strips_in(j) + strips_in(pairs + j):
                copy.start()

        @pl.loop(1, n // 2)
        def _(t):
            for copy in rows_in(right_block(t)) + rows_in(left_block(t)):
                copy.start()

        for copy in rows_in(left_block(n // 2)):
            copy.start()

    def grads(b, c):
        at = (block(b), chunk(c))
        d_hidden = lax.dot_general(dy_v[block(b), :], wd_v[chunk(c), :], NT, preferred_element_type=F32)
        g, u = dg_v[at].astype(F32), du_v[at].astype(F32)
        sig = jax.nn.sigmoid(g)
        act = g * sig
        hid_v[at] = (act * u).astype(BF16)
        dg_v[at] = (d_hidden * u * (sig + act * (1.0 - sig))).astype(BF16)
        du_v[at] = (d_hidden * act).astype(BF16)

    def term(b, s):
        return lax.dot_general(dg_v[block(b), :], wg_v[strip(s), :], NT, preferred_element_type=F32) + lax.dot_general(
            du_v[block(b), :], wu_v[strip(s), :], NT, preferred_element_type=F32
        )

    def target(odd):
        return {"tp": left if odd else right}

    def rs_copy(s, odd, t):
        return pltpu.make_async_remote_copy(
            src_ref=slots.at[s, t],
            dst_ref=slots.at[s, t + 1],
            send_sem=send_sem.at[s],
            recv_sem=rs_sem.at[s, t],
            device_id=target(odd),
            device_id_type=pl.DeviceIdType.MESH,
        )

    def ag_block(odd, t):
        return gather_block(n, me, odd, t)

    def ag_copy(s, odd, t):
        here = dx.at[block(ag_block(odd, t)), strip(s)]
        return ag_to(s, odd, t, here, here)

    def ag_to(s, odd, t, src, dst):
        return pltpu.make_async_remote_copy(
            src_ref=src,
            dst_ref=dst,
            send_sem=send_sem.at[s],
            recv_sem=ag_sem.at[s, t],
            device_id=target(odd),
            device_id_type=pl.DeviceIdType.MESH,
        )

    def ag_last_copy(s, odd):
        t = n - 3
        dst = (tail_left if odd else tail_right).at[:, strip(s - odd * pairs)]
        return ag_to(s, odd, t, dx.at[block(ag_block(odd, t)), strip(s)], dst)

    def send_first(s, odd):
        slots[s, 0] = term(right_block(0), s).astype(BF16)
        rs_copy(s, odd, 0).start()

    def pass_on(s, odd, t):
        rs_copy(s, odd, t - 1).wait_recv()
        b = left_block(t) if odd else right_block(t)
        slots[s, t] = (slots[s, t].astype(F32) + term(b, s)).astype(BF16)
        rs_copy(s, odd, t - 1).wait_send()
        rs_copy(s, odd, t).start()

    def finish(s, odd):
        t = n - 1
        rs_copy(s, odd, t - 1).wait_recv()
        b = left_block(t) if odd else right_block(t)
        dx[block(b), strip(s)] = (slots[s, t].astype(F32) + term(b, s)).astype(BF16)
        rs_copy(s, odd, t - 1).wait_send()
        ag_copy(s, odd, 0).start()

    def hand_on(s, odd, t):
        here = dx.at[block(ag_block(odd, t)), strip(s)]
        arrived = ag_to(s, odd, t - 1, here, here)
        arrived.wait_recv()
        arrived.wait_send()

        @pl.when(t < n - 3)
        def _():
            ag_copy(s, odd, t).start()

        @pl.when(t == n - 3)
        def _():
            ag_last_copy(s, odd).start()

    def down_grad(i):
        dw_down[tile(i), :] = lax.dot_general(hid_v[:, tile(i)], dy_v[...], TN, preferred_element_type=F32).astype(BF16)

    def up_grads(k, i):
        held, first = halves[k]
        xt = held[:, tile(i)]
        at = pl.ds(pl.multiple_of(first + i * TILE, TILE), TILE)
        dw_gate[at, :] = lax.dot_general(xt, dg_v[...], TN, preferred_element_type=F32).astype(BF16)
        dw_up[at, :] = lax.dot_general(xt, du_v[...], TN, preferred_element_type=F32).astype(BF16)

    down_in(1).start()
    first[0].wait()
    down_in(2).start()
    first[1].wait()
    down_in(3).start()

    start_rest()
    first[2].wait()

    @pl.loop(0, CHUNKS)
    def _(c):
        down_in(c).wait()
        grads(right_block(0), c)

    pl.semaphore_wait(barrier, 2)

    @pl.loop(0, pairs)
    def _(j):
        for odd in range(2):
            for copy in strips_in(odd * pairs + j):
                copy.wait()
            send_first(odd * pairs + j, odd)

    def arrive(b):
        for copy in rows_in(b):
            copy.wait()

    arrive(right_block(1))

    @pl.loop(0, CHUNKS)
    def _(c):
        grads(right_block(1), c)

    arrive(left_block(1))

    @pl.loop(0, CHUNKS)
    def _(c):
        grads(left_block(1), c)

    half = n // 2

    @pl.loop(1, half - 1)
    def _(t):
        arrive(right_block(t + 1))
        arrive(left_block(t + 1))

        @pl.loop(0, pairs)
        def _(j):
            pass_on(j, 0, t)
            grads(right_block(t + 1), j)
            pass_on(pairs + j, 1, t)
            grads(left_block(t + 1), j)

    arrive(left_block(half))

    @pl.loop(0, pairs)
    def _(j):
        pass_on(j, 0, half - 1)
        grads(left_block(half), j)
        pass_on(pairs + j, 1, half - 1)

    @pl.loop(half, n - 1)
    def _(t):
        @pl.loop(0, pairs)
        def _(j):
            pass_on(j, 0, t)
            pass_on(pairs + j, 1, t)
            i = (t - half) * pairs + j

            @pl.when(i < hidden // TILE)
            def _():
                down_grad(i)

    @pl.loop(0, pairs)
    def _(j):
        finish(j, 0)
        finish(pairs + j, 1)

    for k in range(2):
        x_in(k).start()

    def hand_on_all(t, also=None):
        @pl.loop(0, pairs)
        def _(j):
            hand_on(j, 0, t)
            hand_on(pairs + j, 1, t)
            if also is not None:
                also(j)

    hand_on_all(1)
    steps = hidden // TILE // pairs
    for k in range(2):
        x_in(k).wait()

        @pl.loop(0, steps)
        def _(t):
            hand_on_all(2 + k * steps + t, also=lambda j: up_grads(k, t * pairs + j))

    @pl.loop(0, pairs)
    def _(j):
        for odd in range(2):
            last = ag_last_copy(odd * pairs + j, odd)
            last.wait_recv()
            last.wait_send()


def gather_block(n, me, odd, t):
    return lax.rem(me + n - 2 + t, n) if odd else lax.rem(me + n - t, n)


def move(pairs_of_refs, sem):
    copies = [pltpu.make_async_copy(src, dst, sem.at[k]) for k, (src, dst) in enumerate(pairs_of_refs)]
    for copy in copies:
        copy.start()
    for copy in copies:
        copy.wait()


def place(n, ref, odd, t):
    rows, cols = ref.shape[0] // n, ref.shape[1] // 2
    b = gather_block(n, lax.axis_index("tp"), odd, t)
    return ref.at[pl.ds(pl.multiple_of(b * rows, rows), rows), pl.ds(odd * cols, cols)]


def write_out(n, dx_v, tail_right, tail_left, dw_gate_v, dw_up_v, dw_down_v, dx, dw_gate, dw_up, dw_down, sem):
    moves = [(dw_gate_v, dw_gate), (dw_up_v, dw_up), (dw_down_v, dw_down)]
    for odd, tail in enumerate((tail_right, tail_left)):
        moves += [(place(n, dx_v, odd, t), place(n, dx, odd, t)) for t in range(n - 2)]
        moves.append((tail, place(n, dx, odd, n - 2)))
    move(moves, sem)


def put_last(n, _, from_left, from_right, dx, sem):
    move([(from_left, place(n, dx, 0, n - 1)), (from_right, place(n, dx, 1, n - 1))], sem)


def solution(mesh):
    n = mesh.shape["tp"]

    def step(x, dy, gate, up, w_gate, w_up, w_down):
        tokens, depth = dy.shape
        hidden = gate.shape[1]
        rows, cols = tokens // n, depth // RINGS
        hbm = pl.BlockSpec(memory_space=pltpu.HBM)
        dma = pltpu.SemaphoreType.DMA
        shapes = [(tokens, depth), (depth, hidden), (depth, hidden), (hidden, depth)]
        tail = (rows, depth // 2)
        vmem = pl.BlockSpec(memory_space=pltpu.VMEM)
        held = pl.pallas_call(
            functools.partial(kernel, n),
            name="mlp_backward",
            out_shape=[pltpu.VMEM(shape, BF16) for shape in (shapes[0], tail, tail, *shapes[1:])],
            in_specs=[hbm] * 7,
            out_specs=[vmem] * 6,
            scratch_shapes=[
                pltpu.VMEM((tokens, depth), BF16),
                pltpu.VMEM((tokens, hidden), BF16),
                pltpu.VMEM((tokens, hidden), BF16),
                pltpu.VMEM((tokens, hidden), BF16),
                pltpu.VMEM((depth, hidden), BF16),
                pltpu.VMEM((depth, hidden), BF16),
                pltpu.VMEM((hidden, depth), BF16),
                pltpu.VMEM((RINGS, n, rows, cols), BF16),
                dma((3, n)),
                dma((CHUNKS,)),
                dma((2, RINGS)),
                dma((2,)),
                dma((RINGS,)),
                dma((RINGS, n)),
                dma((RINGS, n)),
            ],
            compiler_params=pltpu.CompilerParams(
                collective_id=0, has_side_effects=True, vmem_limit_bytes=44_500_000
            ),
            cost_estimate=pl.CostEstimate(
                flops=12 * tokens * depth * hidden, bytes_accessed=14 * tokens * depth * 2, transcendentals=0
            ),
        )(x, dy, gate, up, w_gate, w_up, w_down)
        around = range(n)
        from_left = lax.ppermute(held[1], "tp", [(i, (i + 1) % n) for i in around])
        from_right = lax.ppermute(held[2], "tp", [(i, (i - 1) % n) for i in around])
        dx, *grads = pl.pallas_call(
            functools.partial(write_out, n),
            name="write_out",
            out_shape=[jax.ShapeDtypeStruct(shape, BF16) for shape in shapes],
            in_specs=[vmem] * 6,
            out_specs=[hbm] * 4,
            scratch_shapes=[dma((2 * n + 1,))],
            compiler_params=pltpu.CompilerParams(vmem_limit_bytes=1_000_000),
            cost_estimate=pl.CostEstimate(
                flops=tokens * depth * hidden, bytes_accessed=5 * tokens * depth * 2, transcendentals=0
            ),
        )(*held)
        dx = pl.pallas_call(
            functools.partial(put_last, n),
            name="put_last",
            out_shape=jax.ShapeDtypeStruct(shapes[0], BF16),
            in_specs=[hbm, vmem, vmem],
            out_specs=hbm,
            input_output_aliases={0: 0},
            scratch_shapes=[dma((2,))],
            compiler_params=pltpu.CompilerParams(vmem_limit_bytes=1_000_000),
        )(dx, from_left, from_right)
        return dx, *grads

    tokens, columns, rows = P("dp", None), P(None, "tp"), P("tp", None)
    return jax.shard_map(
        step,
        mesh=mesh,
        in_specs=(tokens, tokens, P("dp", "tp"), P("dp", "tp"), columns, columns, rows),
        out_specs=(tokens, P("dp", "tp"), P("dp", "tp"), P(("dp", "tp"), None)),
        check_vma=False,
    )
```

```python
import functools

import jax
import jax.numpy as jnp
from jax import lax
from jax.experimental import pallas as pl
from jax.experimental.pallas import tpu as pltpu
from jax.sharding import PartitionSpec as P

RINGS = 4
CHUNKS = 4
TILE = 128
BF16, F32 = jnp.bfloat16, jnp.float32
NT = (((1,), (1,)), ((), ()))
TN = (((0,), (0,)), ((), ()))


def kernel(
    n,
    x,
    dy,
    gate,
    up,
    w_gate,
    w_up,
    w_down,
    dx,
    tail_right,
    tail_left,
    dw_gate,
    dw_up,
    dw_down,
    dy_v,
    dg_v,
    du_v,
    hid_v,
    wg_v,
    wu_v,
    wd_v,
    slots,
    in_sem,
    wd_sem,
    w_sem,
    x_sem,
    send_sem,
    rs_sem,
    ag_sem,
):
    tokens, depth = dy.shape
    hidden = gate.shape[1]
    rows, cols, fcols = tokens // n, depth // RINGS, hidden // CHUNKS
    me = lax.axis_index("tp")
    right, left = lax.rem(me + 1, n), lax.rem(me + n - 1, n)

    barrier = pltpu.get_barrier_semaphore()
    for neighbour in (left, right):
        pl.semaphore_signal(barrier, inc=1, device_id={"tp": neighbour}, device_id_type=pl.DeviceIdType.MESH)

    def block(b):
        return pl.ds(pl.multiple_of(b * rows, rows), rows)

    def strip(s):
        return pl.ds(pl.multiple_of(s * cols, cols), cols)

    def chunk(c):
        return pl.ds(pl.multiple_of(c * fcols, fcols), fcols)

    def tile(i):
        return pl.ds(pl.multiple_of(i * TILE, TILE), TILE)

    def rows_in(b):
        return [
            pltpu.make_async_copy(src.at[block(b), :], dst.at[block(b), :], in_sem.at[k, b])
            for k, (src, dst) in enumerate(((gate, dg_v), (up, du_v), (dy, dy_v)))
        ]

    def down_in(c):
        return pltpu.make_async_copy(w_down.at[chunk(c), :], wd_v.at[chunk(c), :], wd_sem.at[c])

    def strips_in(s):
        return [
            pltpu.make_async_copy(src.at[strip(s), :], dst.at[strip(s), :], w_sem.at[k, s])
            for k, (src, dst) in enumerate(((w_gate, wg_v), (w_up, wu_v)))
        ]

    halves = [(wg_v, 0), (wu_v, hidden)]

    def x_in(k):
        dst, first = halves[k]
        return pltpu.make_async_copy(x.at[:, pl.ds(first, hidden)], dst, x_sem.at[k])


    def right_block(t):
        return lax.rem(me + 2 * n - 1 - t, n)

    def left_block(t):
        return lax.rem(me + n - 1 + t, n)

    first = rows_in(right_block(0))
    for copy in first:
        copy.start()
    down_in(0).start()

    pairs = RINGS // 2

    def start_rest():
        @pl.loop(0, pairs)
        def _(j):
            for copy in strips_in(j) + strips_in(pairs + j):
                copy.start()

        @pl.loop(1, n // 2)
        def _(t):
            for copy in rows_in(right_block(t)) + rows_in(left_block(t)):
                copy.start()

        for copy in rows_in(left_block(n // 2)):
            copy.start()

    def grads(b, c):
        at = (block(b), chunk(c))
        d_hidden = lax.dot_general(dy_v[block(b), :], wd_v[chunk(c), :], NT, preferred_element_type=F32)
        g, u = dg_v[at].astype(F32), du_v[at].astype(F32)
        sig = jax.nn.sigmoid(g)
        act = g * sig
        hid_v[at] = (act * u).astype(BF16)
        dg_v[at] = (d_hidden * u * (sig + act * (1.0 - sig))).astype(BF16)
        du_v[at] = (d_hidden * act).astype(BF16)

    def term(b, s):
        return lax.dot_general(dg_v[block(b), :], wg_v[strip(s), :], NT, preferred_element_type=F32) + lax.dot_general(
            du_v[block(b), :], wu_v[strip(s), :], NT, preferred_element_type=F32
        )

    def target(odd):
        return {"tp": left if odd else right}

    def rs_copy(s, odd, t):
        return pltpu.make_async_remote_copy(
            src_ref=slots.at[s, t],
            dst_ref=slots.at[s, t + 1],
            send_sem=send_sem.at[s],
            recv_sem=rs_sem.at[s, t],
            device_id=target(odd),
            device_id_type=pl.DeviceIdType.MESH,
        )

    def ag_block(odd, t):
        return gather_block(n, me, odd, t)

    def ag_copy(s, odd, t):
        here = dx.at[block(ag_block(odd, t)), strip(s)]
        return ag_to(s, odd, t, here, here)

    def ag_to(s, odd, t, src, dst):
        return pltpu.make_async_remote_copy(
            src_ref=src,
            dst_ref=dst,
            send_sem=send_sem.at[s],
            recv_sem=ag_sem.at[s, t],
            device_id=target(odd),
            device_id_type=pl.DeviceIdType.MESH,
        )

    def ag_last_copy(s, odd):
        t = n - 3
        dst = (tail_left if odd else tail_right).at[:, strip(s - odd * pairs)]
        return ag_to(s, odd, t, dx.at[block(ag_block(odd, t)), strip(s)], dst)

    def send_first(s, odd):
        slots[s, 0] = term(right_block(0), s).astype(BF16)
        rs_copy(s, odd, 0).start()

    def pass_on(s, odd, t):
        rs_copy(s, odd, t - 1).wait_recv()
        b = left_block(t) if odd else right_block(t)
        slots[s, t] = (slots[s, t].astype(F32) + term(b, s)).astype(BF16)
        rs_copy(s, odd, t - 1).wait_send()
        rs_copy(s, odd, t).start()

    def finish(s, odd):
        t = n - 1
        rs_copy(s, odd, t - 1).wait_recv()
        b = left_block(t) if odd else right_block(t)
        dx[block(b), strip(s)] = (slots[s, t].astype(F32) + term(b, s)).astype(BF16)
        rs_copy(s, odd, t - 1).wait_send()
        ag_copy(s, odd, 0).start()

    def hand_on(s, odd, t):
        here = dx.at[block(ag_block(odd, t)), strip(s)]
        arrived = ag_to(s, odd, t - 1, here, here)
        arrived.wait_recv()
        arrived.wait_send()

        @pl.when(t < n - 3)
        def _():
            ag_copy(s, odd, t).start()

        @pl.when(t == n - 3)
        def _():
            ag_last_copy(s, odd).start()

    def down_grad(i):
        dw_down[tile(i), :] = lax.dot_general(hid_v[:, tile(i)], dy_v[...], TN, preferred_element_type=F32).astype(BF16)

    def up_grads(k, i):
        held, first = halves[k]
        xt = held[:, tile(i)]
        at = pl.ds(pl.multiple_of(first + i * TILE, TILE), TILE)
        dw_gate[at, :] = lax.dot_general(xt, dg_v[...], TN, preferred_element_type=F32).astype(BF16)
        dw_up[at, :] = lax.dot_general(xt, du_v[...], TN, preferred_element_type=F32).astype(BF16)

    down_in(1).start()
    first[0].wait()
    down_in(2).start()
    first[1].wait()
    down_in(3).start()

    start_rest()
    first[2].wait()

    @pl.loop(0, CHUNKS)
    def _(c):
        down_in(c).wait()
        grads(right_block(0), c)

    pl.semaphore_wait(barrier, 2)

    @pl.loop(0, pairs)
    def _(j):
        for odd in range(2):
            for copy in strips_in(odd * pairs + j):
                copy.wait()
            send_first(odd * pairs + j, odd)

    def arrive(b):
        for copy in rows_in(b):
            copy.wait()

    arrive(right_block(1))

    @pl.loop(0, CHUNKS)
    def _(c):
        grads(right_block(1), c)

    arrive(left_block(1))

    @pl.loop(0, CHUNKS)
    def _(c):
        grads(left_block(1), c)

    half = n // 2

    @pl.loop(1, half - 1)
    def _(t):
        arrive(right_block(t + 1))
        arrive(left_block(t + 1))

        @pl.loop(0, pairs)
        def _(j):
            pass_on(j, 0, t)
            for c in range(CHUNKS // pairs):
                grads(right_block(t + 1), j * (CHUNKS // pairs) + c)
            pass_on(pairs + j, 1, t)
            for c in range(CHUNKS // pairs):
                grads(left_block(t + 1), j * (CHUNKS // pairs) + c)

    arrive(left_block(half))

    @pl.loop(0, pairs)
    def _(j):
        pass_on(j, 0, half - 1)
        for c in range(CHUNKS // pairs):
            grads(left_block(half), j * (CHUNKS // pairs) + c)
        pass_on(pairs + j, 1, half - 1)

    @pl.loop(half, n - 1)
    def _(t):
        @pl.loop(0, pairs)
        def _(j):
            pass_on(j, 0, t)
            pass_on(pairs + j, 1, t)
            i = (t - half) * pairs + j

            @pl.when(i < hidden // TILE // 2)
            def _():
                down_grad(2 * i)
                down_grad(2 * i + 1)

    @pl.loop(0, pairs)
    def _(j):
        finish(j, 0)
        finish(pairs + j, 1)

    for k in range(2):
        x_in(k).start()

    def hand_on_all(t, also=None):
        @pl.loop(0, pairs)
        def _(j):
            hand_on(j, 0, t)
            hand_on(pairs + j, 1, t)
            if also is not None:
                also(j)

    hand_on_all(1)
    steps = hidden // TILE // pairs // 2
    for k in range(2):
        x_in(k).wait()

        @pl.loop(0, steps)
        def _(t):
            hand_on_all(2 + k * steps + t, also=lambda j: [up_grads(k, 2 * (t * pairs + j) + q) for q in range(2)])

    @pl.loop(0, pairs)
    def _(j):
        for odd in range(2):
            last = ag_last_copy(odd * pairs + j, odd)
            last.wait_recv()
            last.wait_send()


def gather_block(n, me, odd, t):
    return lax.rem(me + n - 2 + t, n) if odd else lax.rem(me + n - t, n)


def move(pairs_of_refs, sem):
    copies = [pltpu.make_async_copy(src, dst, sem.at[k]) for k, (src, dst) in enumerate(pairs_of_refs)]
    for copy in copies:
        copy.start()
    for copy in copies:
        copy.wait()


def place(n, ref, odd, t):
    rows, cols = ref.shape[0] // n, ref.shape[1] // 2
    b = gather_block(n, lax.axis_index("tp"), odd, t)
    return ref.at[pl.ds(pl.multiple_of(b * rows, rows), rows), pl.ds(odd * cols, cols)]


def write_out(n, dx_v, tail_right, tail_left, dw_gate_v, dw_up_v, dw_down_v, dx, dw_gate, dw_up, dw_down, sem):
    moves = [(dw_gate_v, dw_gate), (dw_up_v, dw_up), (dw_down_v, dw_down)]
    for odd, tail in enumerate((tail_right, tail_left)):
        moves += [(place(n, dx_v, odd, t), place(n, dx, odd, t)) for t in range(n - 2)]
        moves.append((tail, place(n, dx, odd, n - 2)))
    move(moves, sem)


def put_last(n, _, from_left, from_right, dx, sem):
    move([(from_left, place(n, dx, 0, n - 1)), (from_right, place(n, dx, 1, n - 1))], sem)


def solution(mesh):
    n = mesh.shape["tp"]

    def step(x, dy, gate, up, w_gate, w_up, w_down):
        tokens, depth = dy.shape
        hidden = gate.shape[1]
        rows, cols = tokens // n, depth // RINGS
        hbm = pl.BlockSpec(memory_space=pltpu.HBM)
        dma = pltpu.SemaphoreType.DMA
        shapes = [(tokens, depth), (depth, hidden), (depth, hidden), (hidden, depth)]
        tail = (rows, depth // 2)
        vmem = pl.BlockSpec(memory_space=pltpu.VMEM)
        held = pl.pallas_call(
            functools.partial(kernel, n),
            name="mlp_backward",
            out_shape=[pltpu.VMEM(shape, BF16) for shape in (shapes[0], tail, tail, *shapes[1:])],
            in_specs=[hbm] * 7,
            out_specs=[vmem] * 6,
            scratch_shapes=[
                pltpu.VMEM((tokens, depth), BF16),
                pltpu.VMEM((tokens, hidden), BF16),
                pltpu.VMEM((tokens, hidden), BF16),
                pltpu.VMEM((tokens, hidden), BF16),
                pltpu.VMEM((depth, hidden), BF16),
                pltpu.VMEM((depth, hidden), BF16),
                pltpu.VMEM((hidden, depth), BF16),
                pltpu.VMEM((RINGS, n, rows, cols), BF16),
                dma((3, n)),
                dma((CHUNKS,)),
                dma((2, RINGS)),
                dma((2,)),
                dma((RINGS,)),
                dma((RINGS, n)),
                dma((RINGS, n)),
            ],
            compiler_params=pltpu.CompilerParams(
                collective_id=0, has_side_effects=True, vmem_limit_bytes=44_500_000
            ),
            cost_estimate=pl.CostEstimate(
                flops=12 * tokens * depth * hidden, bytes_accessed=14 * tokens * depth * 2, transcendentals=0
            ),
        )(x, dy, gate, up, w_gate, w_up, w_down)
        around = range(n)
        from_left = lax.ppermute(held[1], "tp", [(i, (i + 1) % n) for i in around])
        from_right = lax.ppermute(held[2], "tp", [(i, (i - 1) % n) for i in around])
        dx, *grads = pl.pallas_call(
            functools.partial(write_out, n),
            name="write_out",
            out_shape=[jax.ShapeDtypeStruct(shape, BF16) for shape in shapes],
            in_specs=[vmem] * 6,
            out_specs=[hbm] * 4,
            scratch_shapes=[dma((2 * n + 1,))],
            compiler_params=pltpu.CompilerParams(vmem_limit_bytes=1_000_000),
            cost_estimate=pl.CostEstimate(
                flops=tokens * depth * hidden, bytes_accessed=5 * tokens * depth * 2, transcendentals=0
            ),
        )(*held)
        dx = pl.pallas_call(
            functools.partial(put_last, n),
            name="put_last",
            out_shape=jax.ShapeDtypeStruct(shapes[0], BF16),
            in_specs=[hbm, vmem, vmem],
            out_specs=hbm,
            input_output_aliases={0: 0},
            scratch_shapes=[dma((2,))],
            compiler_params=pltpu.CompilerParams(vmem_limit_bytes=1_000_000),
        )(dx, from_left, from_right)
        return dx, *grads

    tokens, columns, rows = P("dp", None), P(None, "tp"), P("tp", None)
    return jax.shard_map(
        step,
        mesh=mesh,
        in_specs=(tokens, tokens, P("dp", "tp"), P("dp", "tp"), columns, columns, rows),
        out_specs=(tokens, P("dp", "tp"), P("dp", "tp"), P(("dp", "tp"), None)),
        check_vma=False,
    )
```
